32 devices in a mesh: pts: 8 (over z, y), var: 4 (over x, core).
Axes of the slice: x: 2, y: 2, z: 4, core: 2. Of those that a mesh axis runs over, the one named last changes fastest.
Arguments:
- tensor: bfloat16 [8, 8192, 4096], P(None, 'pts', 'var'), may hold values from -36 to 36
- level_init: float32 [64, 4096], P(None, 'var'), may hold values from -6 to 6
- time_init: float32 [8, 64], replicated, may hold values from -6 to 6
Outputs:
- point_factor: float32 [64, 8192], P(None, 'pts')
- level_factor: float32 [64, 4096], P(None, 'var')
- time_out: float32 [8, 64], replicated
The draws below stay inside these ranges and needn't reach their ends.
All inputs are finite; a program needn't handle non-finite values.
Results may differ from the reference program's by a relative error of at most 0.011.
Values sent between devices are 32-bit elements; how exact they have to be, the bound alone decides.
No kernel may reach another device: no remote copies, remote signals or barrier semaphores. Data moves between devices by JAX's collectives and lax.ppermute only.
A program may use at most 128 MiB of HBM per device.

```python
import math
import jax
import jax.numpy as jnp
from jax import lax

RANK = 64
STEPS = 8
SWEEPS = 3
POINTS = 8192
LEVELS = 4096


def draw_tensor(key, part):
    key_base, key_rows, key_cols = jax.random.split(key, 3)
    row_scale = jnp.exp(jax.random.uniform(key_rows, (1, POINTS, 1), jnp.float32, math.log(0.3), math.log(3.0)))
    col_scale = jnp.exp(jax.random.uniform(key_cols, (1, 1, LEVELS), jnp.float32, math.log(0.3), math.log(3.0)))
    base_vals = jnp.clip(jax.random.normal(key_base, (STEPS, POINTS, LEVELS), jnp.float32), -4.0, 4.0)
    return (base_vals * row_scale * col_scale).astype(jnp.bfloat16)


def block_scale(key, shape, cuts, least, top_value):
    gain, own = 1.0, jax.random.fold_in(key, 6)
    for dim, blocks in cuts:
        draws = jnp.exp(jax.random.uniform(jax.random.fold_in(own, dim), (blocks,), jnp.float32, least / len(cuts), top_value / len(cuts)))
        gain = gain * jnp.repeat(draws, shape[dim] // blocks).reshape([-1 if axis == dim else 1 for axis in range(len(shape))])
    return gain


def bell_draw(stream_key, extent, deviation, most, cuts=(), kind=jnp.bfloat16):
    level = block_scale(stream_key, extent, cuts, -0.22, 0.18) if cuts else 1.0
    entries = jax.random.normal(stream_key, extent, jnp.float32) * deviation * level
    return jnp.minimum(jnp.maximum(entries, -most), most).astype(kind)


def setup_inputs(seed: int = 0) -> dict:
    splits = jax.random.split(jax.random.key(seed), 4)
    tensor = draw_tensor(jax.random.fold_in(splits[3], 71), 0)
    level_init = bell_draw(splits[1], (RANK, LEVELS), 1.0, 6.0, ((1, 4),), jnp.float32)
    time_init = bell_draw(splits[2], (STEPS, RANK), 1.0, 6.0, (), jnp.float32)
    return dict(tensor=tensor, level_init=level_init, time_init=time_init)


HIGH_PRECISION = lax.Precision.HIGHEST
EPSILON = 1e-06

def gram_of(factor):
    return jnp.dot(factor.astype(jnp.float32), factor.T.astype(jnp.float32), precision=HIGH_PRECISION, preferred_element_type=jnp.float32)

def ridge_solve(gram_mat, right_side):
    order_count = gram_mat.shape[0]
    ridge_term = 0.01 * jnp.trace(gram_mat) / order_count + EPSILON
    system = gram_mat + ridge_term * jnp.eye(order_count, dtype=jnp.float32)
    chol_lower = jnp.linalg.cholesky(system)
    middle = lax.linalg.triangular_solve(chol_lower, right_side, left_side=True, lower=True)
    return lax.linalg.triangular_solve(chol_lower, middle, left_side=True, lower=True, transpose_a=True)

def unit_rows(factor, count):
    col_sumsq = lax.optimization_barrier(jnp.sum(factor * factor, axis=1))
    col_scale = 1.0 / jnp.sqrt(col_sumsq / count + EPSILON)
    return factor * col_scale[:, None]

def reference(tensor, level_init, time_init):
    level_factor = level_init
    level_grammat = gram_of(level_init)
    time_factor = time_init
    point_factor = None
    for sweep_index in range(SWEEPS):
        time_gram = jnp.dot(time_factor.T.astype(jnp.float32), time_factor.astype(jnp.float32), precision=HIGH_PRECISION, preferred_element_type=jnp.float32)
        level_bf = level_factor.astype(jnp.bfloat16)
        mttk_point = jnp.zeros((RANK, POINTS), jnp.float32)
        for step_index in range(STEPS):
            product = jnp.einsum('rv,pv->rp', level_bf.astype(jnp.float32), tensor[step_index].astype(jnp.float32), preferred_element_type=jnp.float32)
            mttk_point = mttk_point + time_factor[step_index][:, None] * product
        point_factor = unit_rows(ridge_solve(level_grammat * time_gram, mttk_point), POINTS)
        point_grammat = gram_of(point_factor)
        point_bf = point_factor.astype(jnp.bfloat16)
        mttk_level = jnp.zeros((RANK, LEVELS), jnp.float32)
        contracted = []
        for step_index in range(STEPS):
            product = jnp.dot(point_bf.astype(jnp.float32), tensor[step_index].astype(jnp.float32), preferred_element_type=jnp.float32)
            contracted.append(product)
            mttk_level = mttk_level + time_factor[step_index][:, None] * product
        level_factor = unit_rows(ridge_solve(point_grammat * time_gram, mttk_level), LEVELS)
        level_grammat = gram_of(level_factor)
        mttk_time = jnp.stack([lax.optimization_barrier(jnp.sum(product * level_factor, axis=1)) for product in contracted])
        time_factor = ridge_solve(point_grammat * level_grammat, mttk_time.T).T
    return (point_factor, level_factor, time_factor * math.sqrt(POINTS * LEVELS))
```

```python
import functools
import math

import jax
import jax.numpy as jnp
from jax import lax
from jax.experimental import pallas as pl
from jax.experimental.pallas import tpu as pltpu
from jax.sharding import PartitionSpec as P

SWEEPS = 3
EPSILON = 1e-06
HIGHEST = lax.Precision.HIGHEST
F32 = jnp.float32
LOOK = 4


def exact_dot(a, b, dims=(((1,), (0,)), ((), ()))):
    return lax.dot_general(a, b, dims, precision=HIGHEST, preferred_element_type=F32)


NT = (((1,), (1,)), ((), ()))


def eye_mask(n):
    return lax.broadcasted_iota(jnp.int32, (n, n), 0) == lax.broadcasted_iota(jnp.int32, (n, n), 1)


def diag_row(g):
    return jnp.sum(jnp.where(eye_mask(g.shape[0]), g, 0.0), axis=0, keepdims=True)


def diag_col(g):
    return jnp.sum(jnp.where(eye_mask(g.shape[0]), g, 0.0), axis=1, keepdims=True)


def unit_scales(g, count):
    return (
        1.0 / jnp.sqrt(diag_row(g) / count + EPSILON),
        1.0 / jnp.sqrt(diag_col(g) / count + EPSILON),
    )


def with_ridge(g):
    n = g.shape[0]
    mask = eye_mask(n)
    trace = jnp.sum(jnp.sum(jnp.where(mask, g, 0.0), axis=0, keepdims=True), axis=1, keepdims=True)
    return g + jnp.where(mask, 0.01 * trace / n + EPSILON, 0.0)


def spd_inverse(a):
    n = a.shape[0]
    groups = n // 8
    wide = jnp.concatenate([a, jnp.where(eye_mask(n), 1.0, 0.0)], axis=1)
    width = 2 * n
    sub = lax.broadcasted_iota(jnp.int32, (8, width), 0)
    rows = [wide[8 * g : 8 * g + 8] for g in range(groups)]
    scale = [jnp.zeros((8, width), F32) for _ in range(groups)]
    cols = {}

    def spread(block):
        for m in range(block * LOOK, min(n, (block + 1) * LOOK)):
            cols[m] = [jnp.broadcast_to(rows[g][:, m : m + 1], (8, width)) for g in range(groups)]

    def whole(group, i):
        return jnp.broadcast_to(group[i : i + 1, :], (8, width))

    spread(0)
    for block in range(n // LOOK):
        spread(block + 1)
        for k in range(block * LOOK, (block + 1) * LOOK):
            g0, i0 = divmod(k, 8)
            col = cols.pop(k)
            inv_pivot = 1.0 / whole(col[g0], i0)
            factor = [col[g] * inv_pivot for g in range(groups)]
            factor[g0] = jnp.where(sub == i0, 0.0, factor[g0])
            scale[g0] = jnp.where(sub == i0, inv_pivot, scale[g0])
            for m in sorted(cols):
                entry = whole(col[m // 8], m % 8)
                cols[m] = [cols[m][g] - factor[g] * entry for g in range(groups)]
            pivot_row = whole(rows[g0], i0)
            rows = [rows[g] - factor[g] * pivot_row for g in range(groups)]
    return jnp.concatenate([rows[g] * scale[g] for g in range(groups)], axis=0)[:, n:]


def gram_kernel(level_ref, gram_ref):
    level = level_ref[...]
    gram_ref[...] = exact_dot(level, level, NT)


def point_pass_kernel(level_ref, tensor_ref, out_ref):
    out_ref[0] = lax.dot_general(
        level_ref[...].astype(jnp.bfloat16), tensor_ref[0], NT, preferred_element_type=F32
    )


def combine(time_cols, parts_ref, out_ref):
    total = time_cols[:, 0:1] * parts_ref[0]
    for k in range(1, parts_ref.shape[0]):
        total = total + time_cols[:, k : k + 1] * parts_ref[k]
    out_ref[...] = total


def first_combine_kernel(gram_ref, time_ref, time_cols_ref, parts_ref, out_ref, tgram_ref, system_ref):
    time = time_ref[...]
    tgram = exact_dot(time, time, (((0,), (0,)), ((), ())))
    tgram_ref[...] = tgram
    system_ref[...] = with_ridge(gram_ref[...] * tgram)
    combine(time_cols_ref[...], parts_ref, out_ref)


def combine_kernel(gram_ref, scale_ref, inverse_ref, mine_ref, other_ref, parts_ref, out_ref, tgram_ref, system_ref, time_ref):
    products = (mine_ref[...] + other_ref[...]) * scale_ref[0:1]
    inverse = inverse_ref[...]
    time = exact_dot(products, inverse)
    time_cols = exact_dot(inverse, products, NT)
    time_ref[...] = time
    tgram = exact_dot(time_cols, time_cols, NT)
    tgram_ref[...] = tgram
    system_ref[...] = with_ridge(gram_ref[...] * tgram)
    level_col = scale_ref[1:2]
    combine(time_cols * jnp.transpose(jnp.broadcast_to(level_col, (8, level_col.shape[1])))[:, 0:1], parts_ref, out_ref)


def last_time_kernel(scale_ref, inverse_ref, mine_ref, other_ref, time_ref, *, factor):
    products = (mine_ref[...] + other_ref[...]) * scale_ref[0:1]
    time_ref[...] = exact_dot(products, inverse_ref[...]) * factor


def inverse_kernel(system_ref, out_ref):
    out_ref[...] = spd_inverse(system_ref[...])


def level_pass_kernel(inverse_ref, mine_ref, other_ref, time_cols_ref, tensor_ref, solved_ref, parts_ref, lo_ref, hi_ref, rounded):
    k = pl.program_id(0)
    half = lo_ref.shape[1]

    @pl.when(k == 0)
    def _():
        solved = exact_dot(inverse_ref[...], mine_ref[...] + other_ref[...])
        solved_ref[...] = solved
        rounded[...] = solved.astype(jnp.bfloat16)
        gram = exact_dot(solved, solved, NT)
        hi_ref[:, half:] = jnp.concatenate([gram, jnp.zeros_like(gram)], axis=1)

    product = jnp.dot(rounded[...], tensor_ref[0], preferred_element_type=F32)
    parts_ref[0] = product
    weighted = time_cols_ref[0] * product

    @pl.when(k == 0)
    def _():
        lo_ref[...] = weighted[:, :half]
        hi_ref[:, :half] = weighted[:, half:]

    @pl.when(k > 0)
    def _():
        lo_ref[...] += weighted[:, :half]
        hi_ref[:, :half] += weighted[:, half:]


def level_solve_kernel(lo_ref, lo2_ref, hi_ref, hi2_ref, tgram_ref, parts_ref, solved_ref, small_ref, pgram_ref, pscale_ref, *, count):
    n = lo_ref.shape[0]
    half = lo_ref.shape[1]
    raw = hi_ref[:, half : half + n] + hi2_ref[:, half : half + n]
    row, col = unit_scales(raw, count)
    pgram = col * raw * row
    pgram_ref[...] = pgram
    pscale_ref[...] = jnp.concatenate([row, jnp.transpose(jnp.broadcast_to(col, (n, n)))[0:1]], axis=0)
    weights = spd_inverse(with_ridge(pgram * tgram_ref[...])) * row
    solved_ref[:, :half] = exact_dot(weights, lo_ref[...] + lo2_ref[...])
    solved_ref[:, half:] = exact_dot(weights, hi_ref[:, :half] + hi2_ref[:, :half])
    solved = solved_ref[...]
    small_ref[0:n] = exact_dot(solved, solved, NT)
    for k in range(parts_ref.shape[0]):
        col_sum = jnp.sum(parts_ref[k] * solved, axis=1, keepdims=True)
        small_ref[n + k : n + k + 1] = jnp.transpose(jnp.broadcast_to(col_sum, (n, n)))[0:1]


def time_inverse_kernel(small_ref, small2_ref, pgram_ref, pscale_ref, gram_ref, scale_ref, inverse_ref, products_ref, *, count):
    n = pgram_ref.shape[0]
    raw = small_ref[0:n] + small2_ref[0:n]
    row, col = unit_scales(raw, count)
    gram = col * raw * row
    gram_ref[...] = gram
    scale_ref[...] = jnp.concatenate([row * pscale_ref[0:1], row], axis=0)
    products_ref[...] = small_ref[n:] + small2_ref[n:]
    inverse_ref[...] = spd_inverse(with_ridge(pgram_ref[...] * gram))


def shape(*dims):
    return jax.ShapeDtypeStruct(dims, F32)


def call(kernel, outs, *args, name, flops=10**6):
    return pl.pallas_call(
        kernel,
        out_shape=outs,
        name=name,
        cost_estimate=pl.CostEstimate(flops=flops, bytes_accessed=10**6, transcendentals=0),
        compiler_params=pltpu.CompilerParams(vmem_limit_bytes=24 << 20),
    )(*args)


def swap(x, axis, mask):
    n = lax.axis_size(axis)
    return lax.ppermute(x, axis, [(i, i ^ mask) for i in range(n)])


def masks_of(n):
    return [1 << i for i in range(n.bit_length() - 1)]


def per_device(tensor, level_init, time_init):
    steps, points, levels = tensor.shape
    rank = level_init.shape[0]
    npts, nvar = lax.axis_size("pts"), lax.axis_size("var")
    points_all, levels_all = points * npts, levels * nvar
    pts_masks, var_masks = masks_of(npts), masks_of(nvar)
    flops = 2 * steps * points * levels * rank

    def sum_but_last(x, axis, masks):
        for mask in masks[:-1]:
            x = x + swap(x, axis, mask)
        return x, swap(x, axis, masks[-1])

    def point_pass(level):
        return pl.pallas_call(
            point_pass_kernel,
            grid=(steps,),
            in_specs=[
                pl.BlockSpec((rank, levels), lambda k: (0, 0)),
                pl.BlockSpec((1, points, levels), lambda k: (k, 0, 0)),
            ],
            out_specs=pl.BlockSpec((1, rank, points), lambda k: (k, 0, 0)),
            out_shape=shape(steps, rank, points),
            name="point_pass",
            cost_estimate=pl.CostEstimate(flops=flops, bytes_accessed=2 * tensor.size, transcendentals=0),
            compiler_params=pltpu.CompilerParams(vmem_limit_bytes=24 << 20),
        )(level, tensor)

    def level_pass(inverse, mine, other, time_cols):
        half = levels // 2
        return pl.pallas_call(
            level_pass_kernel,
            grid=(steps,),
            in_specs=[
                pl.BlockSpec((rank, rank), lambda k: (0, 0)),
                pl.BlockSpec((rank, points), lambda k: (0, 0)),
                pl.BlockSpec((rank, points), lambda k: (0, 0)),
                pl.BlockSpec((1, rank, 1), lambda k: (k, 0, 0)),
                pl.BlockSpec((1, points, levels), lambda k: (k, 0, 0)),
            ],
            out_specs=[
                pl.BlockSpec((rank, points), lambda k: (0, 0)),
                pl.BlockSpec((1, rank, levels), lambda k: (k, 0, 0)),
                pl.BlockSpec((rank, half), lambda k: (0, 0)),
                pl.BlockSpec((rank, half + 2 * rank), lambda k: (0, 0)),
            ],
            out_shape=[
                shape(rank, points),
                shape(steps, rank, levels),
                shape(rank, half),
                shape(rank, half + 2 * rank),
            ],
            scratch_shapes=[pltpu.VMEM((rank, points), jnp.bfloat16)],
            name="level_pass",
            cost_estimate=pl.CostEstimate(flops=flops, bytes_accessed=2 * tensor.size, transcendentals=0),
            compiler_params=pltpu.CompilerParams(vmem_limit_bytes=24 << 20),
        )(inverse, mine, other, time_cols, tensor)

    gram0 = call(gram_kernel, shape(rank, rank), level_init, name="level_gram")
    gram, gram_other = sum_but_last(gram0, "var", var_masks)
    gram = gram + gram_other
    parts = point_pass(level_init)
    time = time_init
    mine, tgram, system = call(
        first_combine_kernel,
        [shape(rank, points), shape(rank, rank), shape(rank, rank)],
        gram, time, time.T, parts,
        name="first_combine",
    )
    for sweep in range(SWEEPS):
        mine, other = sum_but_last(mine, "var", var_masks)
        inverse = call(inverse_kernel, shape(rank, rank), system, name="point_inverse", flops=10**7)
        point_solved, parts, lo, hi = level_pass(inverse, mine, other, time[:, :, None])
        order = pts_masks
        if len(pts_masks) > 2:
            flipped = [pts_masks[1], pts_masks[0]] + pts_masks[2:]
        else:
            flipped = pts_masks[::-1]
        for a, b in zip(order[:-1], flipped[:-1]):
            lo2, hi2 = swap(lo, "pts", a), swap(hi, "pts", b)
            lo, hi = lo + lo2, hi + hi2
        lo2, hi2 = swap(lo, "pts", order[-1]), swap(hi, "pts", flipped[-1])
        level_solved, small, pgram, pscale = call(
            functools.partial(level_solve_kernel, count=points_all),
            [shape(rank, levels), shape(rank + steps, rank), shape(rank, rank), shape(2, rank)],
            lo, lo2, hi, hi2, tgram, parts,
            name="level_solve",
        )
        small, small2 = sum_but_last(small, "var", var_masks)
        gram, scale, inverse, products = call(
            functools.partial(time_inverse_kernel, count=levels_all),
            [shape(rank, rank), shape(2, rank), shape(rank, rank), shape(steps, rank)],
            small, small2, pgram, pscale,
            name="time_inverse", flops=10**7,
        )
        products, products2 = sum_but_last(products, "pts", pts_masks)
        if sweep + 1 < SWEEPS:
            parts = point_pass(level_solved)
            mine, tgram, system, time = call(
                combine_kernel,
                [shape(rank, points), shape(rank, rank), shape(rank, rank), shape(steps, rank)],
                gram, scale, inverse, products, products2, parts,
                name="combine",
            )
        else:
            time_out = call(
                functools.partial(last_time_kernel, factor=math.sqrt(points_all * levels_all)),
                shape(steps, rank),
                scale, inverse, products, products2,
                name="last_time",
            )
    return (point_solved * pscale[0][:, None], level_solved * scale[1][:, None], time_out)


def solution(mesh):
    placed = (P(None, "pts", "var"), P(None, "var"), P())
    return jax.shard_map(
        per_device,
        mesh=mesh,
        in_specs=placed,
        out_specs=(P(None, "pts"), P(None, "var"), P()),
        check_vma=False,
    )
```

```python
import functools
import math

import jax
import jax.numpy as jnp
from jax import lax
from jax.experimental import pallas as pl
from jax.experimental.pallas import tpu as pltpu
from jax.sharding import PartitionSpec as P


SWEEPS = 3
EPSILON = 1e-06
HIGHEST = lax.Precision.HIGHEST
F32 = jnp.float32
LOOK = 4
PIECES = (2, 6)


def exact_dot(a, b, dims=(((1,), (0,)), ((), ()))):
    return lax.dot_general(a, b, dims, precision=HIGHEST, preferred_element_type=F32)


NT = (((1,), (1,)), ((), ()))


def eye_mask(n):
    return lax.broadcasted_iota(jnp.int32, (n, n), 0) == lax.broadcasted_iota(jnp.int32, (n, n), 1)


def diag_row(g):
    return jnp.sum(jnp.where(eye_mask(g.shape[0]), g, 0.0), axis=0, keepdims=True)


def diag_col(g):
    return jnp.sum(jnp.where(eye_mask(g.shape[0]), g, 0.0), axis=1, keepdims=True)


def unit_scales(g, count):
    return (
        1.0 / jnp.sqrt(diag_row(g) / count + EPSILON),
        1.0 / jnp.sqrt(diag_col(g) / count + EPSILON),
    )


def with_ridge(g):
    n = g.shape[0]
    mask = eye_mask(n)
    trace = jnp.sum(jnp.sum(jnp.where(mask, g, 0.0), axis=0, keepdims=True), axis=1, keepdims=True)
    return g + jnp.where(mask, 0.01 * trace / n + EPSILON, 0.0)


def spd_inverse(a):
    n = a.shape[0]
    groups = n // 8
    wide = jnp.concatenate([a, jnp.where(eye_mask(n), 1.0, 0.0)], axis=1)
    width = 2 * n
    sub = lax.broadcasted_iota(jnp.int32, (8, width), 0)
    rows = [wide[8 * g : 8 * g + 8] for g in range(groups)]
    scale = [jnp.zeros((8, width), F32) for _ in range(groups)]
    cols = {}

    def spread(block):
        for m in range(block * LOOK, min(n, (block + 1) * LOOK)):
            cols[m] = [jnp.broadcast_to(rows[g][:, m : m + 1], (8, width)) for g in range(groups)]

    def whole(group, i):
        return jnp.broadcast_to(group[i : i + 1, :], (8, width))

    spread(0)
    for block in range(n // LOOK):
        spread(block + 1)
        for k in range(block * LOOK, (block + 1) * LOOK):
            g0, i0 = divmod(k, 8)
            col = cols.pop(k)
            inv_pivot = 1.0 / whole(col[g0], i0)
            factor = [col[g] * inv_pivot for g in range(groups)]
            factor[g0] = jnp.where(sub == i0, 0.0, factor[g0])
            scale[g0] = jnp.where(sub == i0, inv_pivot, scale[g0])
            for m in sorted(cols):
                entry = whole(col[m // 8], m % 8)
                cols[m] = [cols[m][g] - factor[g] * entry for g in range(groups)]
            pivot_row = whole(rows[g0], i0)
            rows = [rows[g] - factor[g] * pivot_row for g in range(groups)]
    return jnp.concatenate([rows[g] * scale[g] for g in range(groups)], axis=0)[:, n:]


def gram_kernel(level_ref, gram_ref):
    level = level_ref[...]
    gram_ref[...] = exact_dot(level, level, NT)


def point_pass_kernel(level_ref, tensor_ref, out_ref, *, first):
    rounded = level_ref[...].astype(jnp.bfloat16)
    for k in range(out_ref.shape[0]):
        out_ref[k] = lax.dot_general(rounded, tensor_ref[first + k], NT, preferred_element_type=F32)


def combine(time_cols, parts_refs, out_ref):
    total, k = None, 0
    for parts_ref in parts_refs:
        for i in range(parts_ref.shape[0]):
            term = time_cols[:, k : k + 1] * parts_ref[i]
            total = term if total is None else total + term
            k += 1
    out_ref[...] = total


def first_combine_kernel(gram_ref, time_ref, time_cols_ref, *refs):
    *parts_refs, out_ref, tgram_ref, system_ref = refs
    time = time_ref[...]
    tgram = exact_dot(time, time, (((0,), (0,)), ((), ())))
    tgram_ref[...] = tgram
    system_ref[...] = with_ridge(gram_ref[...] * tgram)
    combine(time_cols_ref[...], parts_refs, out_ref)


def combine_kernel(gram_ref, scale_ref, inverse_ref, mine_ref, other_ref, *refs):
    *parts_refs, out_ref, tgram_ref, system_ref, time_ref = refs
    inverse = inverse_ref[...]
    products = (mine_ref[...] + other_ref[...]) * scale_ref[0:1]
    time_ref[...] = exact_dot(products, inverse)
    time_cols = exact_dot(inverse, products, NT)
    tgram = exact_dot(time_cols, time_cols, NT)
    tgram_ref[...] = tgram
    system_ref[...] = with_ridge(gram_ref[...] * tgram)
    level_row = scale_ref[1:2]
    level_col = jnp.transpose(jnp.broadcast_to(level_row, (8, level_row.shape[1])))[:, 0:1]
    combine(time_cols * level_col, parts_refs, out_ref)


def last_time_kernel(scale_ref, inverse_ref, mine_ref, other_ref, time_ref, *, factor):
    products = (mine_ref[...] + other_ref[...]) * scale_ref[0:1]
    time_ref[...] = exact_dot(products, inverse_ref[...]) * factor


def slab_copies(tensor_ref, held_ref, sems):
    copies = [pltpu.make_async_copy(tensor_ref.at[k], held_ref.at[k], sems.at[k]) for k in range(held_ref.shape[0])]
    for copy in copies:
        copy.start()
    return copies


def inverse_kernel(system_ref, tensor_ref, out_ref, held_ref, sems):
    copies = slab_copies(tensor_ref, held_ref, sems)
    out_ref[...] = spd_inverse(system_ref[...])
    for copy in copies:
        copy.wait()


def first_pass_kernel(level_ref, tensor_ref, out_ref, held, sems):
    copies = slab_copies(tensor_ref, held, sems)
    rounded = level_ref[...].astype(jnp.bfloat16)
    for k, copy in enumerate(copies):
        copy.wait()
        out_ref[k] = lax.dot_general(rounded, held[k], NT, preferred_element_type=F32)


def level_pass_kernel(
    side_ref, inverse_ref, mine_ref, other_ref, time_cols_ref, tensor_ref, solved_ref, parts_ref, keep_ref, send_ref, sums
):
    half = sums.shape[2]
    solved = exact_dot(inverse_ref[...], mine_ref[...] + other_ref[...])
    solved_ref[...] = solved
    rounded = solved.astype(jnp.bfloat16)
    gram = exact_dot(solved, solved, NT)
    gram = jnp.concatenate([gram, jnp.zeros_like(gram)], axis=1)
    keep_ref[:, half:] = gram
    send_ref[:, half:] = gram
    for k in range(tensor_ref.shape[0]):
        product = jnp.dot(rounded, tensor_ref[k], preferred_element_type=F32)
        parts_ref[k] = product
        weighted = time_cols_ref[:, k : k + 1] * product
        for i in range(2):
            piece = weighted[:, i * half : (i + 1) * half]
            sums[i] = piece if k == 0 else sums[i] + piece
    side = side_ref[0]
    keep_ref[:, :half] = sums[side]
    send_ref[:, :half] = sums[1 - side]


def level_weights_kernel(mine_ref, tgram_ref, weights_ref, pgram_ref, pscale_ref, *, count):
    n = tgram_ref.shape[0]
    half = mine_ref.shape[1] - 2 * n
    raw = mine_ref[:, half : half + n]
    row, col = unit_scales(raw, count)
    pgram = col * raw * row
    pgram_ref[...] = pgram
    pscale_ref[...] = row
    weights_ref[...] = spd_inverse(with_ridge(pgram * tgram_ref[...])) * row


def level_solve_kernel(side_ref, weights_ref, mine_ref, other_ref, parts_ref, solved_ref, small_ref):
    n = weights_ref.shape[0]
    half = solved_ref.shape[1] // 2
    side = side_ref[0]
    weights = weights_ref[...]
    solved_ref[:, pl.ds(pl.multiple_of(side * half, half), half)] = exact_dot(weights, mine_ref[:, :half])
    solved_ref[:, pl.ds(pl.multiple_of((1 - side) * half, half), half)] = exact_dot(weights, other_ref[:, :half])
    solved = solved_ref[...]
    small_ref[0:n] = exact_dot(solved, solved, NT)
    for k in range(parts_ref.shape[0]):
        col_sum = jnp.sum(parts_ref[k] * solved, axis=1, keepdims=True)
        small_ref[n + k : n + k + 1] = jnp.transpose(jnp.broadcast_to(col_sum, (n, n)))[0:1]


def time_inverse_kernel(small_ref, pgram_ref, pscale_ref, gram_ref, scale_ref, inverse_ref, *, count):
    n = pgram_ref.shape[0]
    raw = small_ref[0:n]
    row, col = unit_scales(raw, count)
    gram = col * raw * row
    gram_ref[...] = gram
    scale_ref[...] = jnp.concatenate([row * pscale_ref[...], row], axis=0)
    inverse_ref[...] = spd_inverse(with_ridge(pgram_ref[...] * gram))


def shape(*dims):
    return jax.ShapeDtypeStruct(dims, F32)


def call(kernel, outs, *args, flops=10**6, spaces=None, limit=8, scratch=()):
    spaces = spaces or [pltpu.VMEM] * len(args)
    return pl.pallas_call(
        kernel,
        out_shape=outs,
        in_specs=[pl.BlockSpec(memory_space=space) for space in spaces],
        out_specs=[pl.BlockSpec(memory_space=pltpu.VMEM)] * len(outs),
        scratch_shapes=scratch,
        cost_estimate=pl.CostEstimate(flops=flops, bytes_accessed=10**6, transcendentals=0),
        compiler_params=pltpu.CompilerParams(vmem_limit_bytes=limit << 20),
    )(*args)


def swap(x, axis, mask):
    n = lax.axis_size(axis)
    return lax.ppermute(x, axis, [(i, i ^ mask) for i in range(n)])


def masks_of(n):
    return [1 << i for i in range(n.bit_length() - 1)]


def per_device(tensor, level_init, time_init):
    steps, points, levels = tensor.shape
    rank = level_init.shape[0]
    npts, nvar = lax.axis_size("pts"), lax.axis_size("var")
    points_all, levels_all = points * npts, levels * nvar
    pts_masks, var_masks = masks_of(npts), masks_of(nvar)
    half = levels // 2
    flops = 2 * steps * points * levels * rank
    V, S = pltpu.VMEM, pltpu.SMEM
    dma_sems = pltpu.SemaphoreType.DMA((steps,))
    square = shape(rank, rank)
    tensor_hbm = pltpu.with_memory_space_constraint(tensor, pltpu.HBM)
    side = (lax.axis_index("pts") & 1).astype(jnp.int32)[None]

    def sum_over(x, axis, masks):
        for mask in masks:
            x = x + swap(x, axis, mask)
        return x

    (gram,) = call(gram_kernel, [square], level_init)
    gram = sum_over(gram, "var", var_masks)
    (first,) = call(
        first_pass_kernel, [shape(steps, rank, points)], level_init, tensor_hbm,
        flops=flops, limit=24, spaces=[V, pltpu.HBM],
        scratch=[V(tensor.shape, tensor.dtype), dma_sems],
    )
    time = time_init
    mine, tgram, system = call(first_combine_kernel, [shape(rank, points), square, square], gram, time, time.T, first)
    for sweep in range(SWEEPS):
        mine = sum_over(mine, "var", var_masks[:-1])
        other = swap(mine, "var", var_masks[-1])
        inverse, held = call(
            inverse_kernel, [square, V(tensor.shape, tensor.dtype)], system, tensor_hbm,
            flops=flops, limit=24, spaces=[V, pltpu.HBM], scratch=[dma_sems],
        )
        held = pltpu.with_memory_space_constraint(held, V)
        point_solved, parts, keep, send = call(
            level_pass_kernel,
            [shape(rank, points), shape(steps, rank, levels)] + [shape(rank, half + 2 * rank)] * 2,
            side, inverse, mine, other, time.T, held,
            flops=flops, limit=24, spaces=[S] + [V] * 5,
            scratch=[V((2, rank, half), F32)],
        )
        keep = keep + swap(send, "pts", pts_masks[0])
        keep = sum_over(keep, "pts", pts_masks[1:])
        other = swap(keep, "pts", pts_masks[0])
        weights, pgram, pscale = call(
            functools.partial(level_weights_kernel, count=points_all),
            [square, square, shape(1, rank)], keep, tgram,
            flops=10**7,
        )
        level_solved, small = call(
            level_solve_kernel, [shape(rank, levels), shape(rank + steps, rank)],
            side, weights, keep, other, parts,
            spaces=[S] + [V] * 4,
        )
        small = sum_over(small, "var", var_masks)
        products = small[rank:]
        gram, scale, inverse = call(
            functools.partial(time_inverse_kernel, count=levels_all),
            [square, shape(2, rank), square], small, pgram, pscale,
            flops=10**7,
        )
        for i, mask in enumerate(pts_masks):
            products2 = swap(products, "pts", mask)
            if i + 1 < len(pts_masks):
                products = products + products2
        if sweep + 1 < SWEEPS:
            pieces, first = [], 0
            for count in PIECES:
                pieces += call(
                    functools.partial(point_pass_kernel, first=first), [shape(count, rank, points)],
                    level_solved, held,
                    flops=flops * count // steps, limit=24,
                )
                first += count
            mine, tgram, system, time = call(
                combine_kernel, [shape(rank, points), square, square, shape(steps, rank)],
                gram, scale, inverse, products, products2, *pieces,
            )
    (time_out,) = call(
        functools.partial(last_time_kernel, factor=math.sqrt(points_all * levels_all)), [shape(steps, rank)],
        scale, inverse, products, products2,
    )
    return (point_solved * pscale[0][:, None], level_solved * scale[1][:, None], time_out)


def solution(mesh):
    placed = (P(None, "pts", "var"), P(None, "var"), P())
    return jax.shard_map(
        per_device,
        mesh=mesh,
        in_specs=placed,
        out_specs=(P(None, "pts"), P(None, "var"), P()),
        check_vma=False,
    )
```

```python
import functools
import math

import jax
import jax.numpy as jnp
from jax import lax
from jax.experimental import pallas as pl
from jax.experimental.pallas import tpu as pltpu
from jax.sharding import PartitionSpec as P


SWEEPS = 3
EPSILON = 1e-06
HIGHEST = lax.Precision.HIGHEST
F32 = jnp.float32
LOOK = 4
PIECES = (1, 2, 5)


def exact_dot(a, b, dims=(((1,), (0,)), ((), ()))):
    return lax.dot_general(a, b, dims, precision=HIGHEST, preferred_element_type=F32)


NT = (((1,), (1,)), ((), ()))


def eye_mask(n):
    return lax.broadcasted_iota(jnp.int32, (n, n), 0) == lax.broadcasted_iota(jnp.int32, (n, n), 1)


def diag_row(g):
    return jnp.sum(jnp.where(eye_mask(g.shape[0]), g, 0.0), axis=0, keepdims=True)


def diag_col(g):
    return jnp.sum(jnp.where(eye_mask(g.shape[0]), g, 0.0), axis=1, keepdims=True)


def unit_scales(g, count):
    return (
        1.0 / jnp.sqrt(diag_row(g) / count + EPSILON),
        1.0 / jnp.sqrt(diag_col(g) / count + EPSILON),
    )


def with_ridge(g):
    n = g.shape[0]
    mask = eye_mask(n)
    trace = jnp.sum(jnp.sum(jnp.where(mask, g, 0.0), axis=0, keepdims=True), axis=1, keepdims=True)
    return g + jnp.where(mask, 0.01 * trace / n + EPSILON, 0.0)


def spd_inverse(a):
    n = a.shape[0]
    groups = n // 8
    wide = jnp.concatenate([a, jnp.where(eye_mask(n), 1.0, 0.0)], axis=1)
    width = 2 * n
    sub = lax.broadcasted_iota(jnp.int32, (8, width), 0)
    rows = [wide[8 * g : 8 * g + 8] for g in range(groups)]
    scale = [jnp.zeros((8, width), F32) for _ in range(groups)]
    cols = {}

    def spread(block):
        for m in range(block * LOOK, min(n, (block + 1) * LOOK)):
            cols[m] = [jnp.broadcast_to(rows[g][:, m : m + 1], (8, width)) for g in range(groups)]

    def whole(group, i):
        return jnp.broadcast_to(group[i : i + 1, :], (8, width))

    spread(0)
    for block in range(n // LOOK):
        spread(block + 1)
        for k in range(block * LOOK, (block + 1) * LOOK):
            g0, i0 = divmod(k, 8)
            col = cols.pop(k)
            inv_pivot = 1.0 / whole(col[g0], i0)
            factor = [col[g] * inv_pivot for g in range(groups)]
            factor[g0] = jnp.where(sub == i0, 0.0, factor[g0])
            scale[g0] = jnp.where(sub == i0, inv_pivot, scale[g0])
            for m in sorted(cols):
                entry = whole(col[m // 8], m % 8)
                cols[m] = [cols[m][g] - factor[g] * entry for g in range(groups)]
            pivot_row = whole(rows[g0], i0)
            rows = [rows[g] - factor[g] * pivot_row for g in range(groups)]
    return jnp.concatenate([rows[g] * scale[g] for g in range(groups)], axis=0)[:, n:]


def gram_kernel(level_ref, gram_ref):
    level = level_ref[...]
    gram_ref[...] = exact_dot(level, level, NT)


def point_pass_kernel(level_ref, tensor_ref, out_ref, *, first):
    rounded = level_ref[...].astype(jnp.bfloat16)
    for k in range(out_ref.shape[0]):
        out_ref[k] = lax.dot_general(rounded, tensor_ref[first + k], NT, preferred_element_type=F32)


def combine(time_cols, parts_refs, out_ref):
    total, k = None, 0
    for parts_ref in parts_refs:
        for i in range(parts_ref.shape[0]):
            term = time_cols[:, k : k + 1] * parts_ref[i]
            total = term if total is None else total + term
            k += 1
    out_ref[...] = total


def first_combine_kernel(gram_ref, time_ref, time_cols_ref, *refs):
    *parts_refs, out_ref, tgram_ref, system_ref = refs
    time = time_ref[...]
    tgram = exact_dot(time, time, (((0,), (0,)), ((), ())))
    tgram_ref[...] = tgram
    system_ref[...] = with_ridge(gram_ref[...] * tgram)
    combine(time_cols_ref[...], parts_refs, out_ref)


def combine_kernel(gram_ref, scale_ref, inverse_ref, mine_ref, other_ref, *refs):
    *parts_refs, out_ref, tgram_ref, system_ref, time_ref = refs
    inverse = inverse_ref[...]
    products = (mine_ref[...] + other_ref[...]) * scale_ref[0:1]
    time_ref[...] = exact_dot(products, inverse)
    time_cols = exact_dot(inverse, products, NT)
    tgram = exact_dot(time_cols, time_cols, NT)
    tgram_ref[...] = tgram
    system_ref[...] = with_ridge(gram_ref[...] * tgram)
    level_row = scale_ref[1:2]
    level_col = jnp.transpose(jnp.broadcast_to(level_row, (8, level_row.shape[1])))[:, 0:1]
    combine(time_cols * level_col, parts_refs, out_ref)


def last_time_kernel(scale_ref, inverse_ref, mine_ref, other_ref, time_ref, *, factor):
    products = (mine_ref[...] + other_ref[...]) * scale_ref[0:1]
    time_ref[...] = exact_dot(products, inverse_ref[...]) * factor


def slab_copies(tensor_ref, held_ref, sems):
    copies = [pltpu.make_async_copy(tensor_ref.at[k], held_ref.at[k], sems.at[k]) for k in range(held_ref.shape[0])]
    for copy in copies:
        copy.start()
    return copies


def inverse_kernel(system_ref, tensor_ref, out_ref, held_ref, sems):
    copies = slab_copies(tensor_ref, held_ref, sems)
    out_ref[...] = spd_inverse(system_ref[...])
    for copy in copies:
        copy.wait()


def first_pass_kernel(level_ref, tensor_ref, out_ref, held, sems):
    copies = slab_copies(tensor_ref, held, sems)
    rounded = level_ref[...].astype(jnp.bfloat16)
    for k, copy in enumerate(copies):
        copy.wait()
        out_ref[k] = lax.dot_general(rounded, held[k], NT, preferred_element_type=F32)


def level_pass_kernel(
    side_ref, inverse_ref, mine_ref, other_ref, time_cols_ref, tensor_ref, solved_ref, parts_ref, keep_ref, send_ref, sums
):
    n = inverse_ref.shape[0]
    half = sums.shape[2]
    solved = exact_dot(inverse_ref[...], mine_ref[...] + other_ref[...])
    solved_ref[...] = solved
    rounded = solved.astype(jnp.bfloat16)
    gram = exact_dot(solved, solved, NT)
    packed = jnp.concatenate([gram[8 * b : 8 * b + 8] for b in range(n // 8)], axis=1)
    keep_ref[n:] = packed
    send_ref[n:] = packed
    for k in range(tensor_ref.shape[0]):
        product = jnp.dot(rounded, tensor_ref[k], preferred_element_type=F32)
        parts_ref[k] = product
        weighted = time_cols_ref[:, k : k + 1] * product
        for i in range(2):
            piece = weighted[:, i * half : (i + 1) * half]
            sums[i] = piece if k == 0 else sums[i] + piece
    side = side_ref[0]
    keep_ref[:n] = sums[side]
    send_ref[:n] = sums[1 - side]


def level_weights_kernel(mine_ref, tgram_ref, weights_ref, pgram_ref, pscale_ref, *, count):
    n = tgram_ref.shape[0]
    raw = jnp.concatenate([mine_ref[n:, n * b : n * b + n] for b in range(n // 8)], axis=0)
    row, col = unit_scales(raw, count)
    pgram = col * raw * row
    pgram_ref[...] = pgram
    pscale_ref[...] = row
    weights_ref[...] = spd_inverse(with_ridge(pgram * tgram_ref[...])) * row


def level_solve_kernel(side_ref, weights_ref, mine_ref, other_ref, parts_ref, solved_ref, small_ref):
    n = weights_ref.shape[0]
    half = solved_ref.shape[1] // 2
    side = side_ref[0]
    weights = weights_ref[...]
    solved_ref[:, pl.ds(pl.multiple_of(side * half, half), half)] = exact_dot(weights, mine_ref[:n])
    solved_ref[:, pl.ds(pl.multiple_of((1 - side) * half, half), half)] = exact_dot(weights, other_ref[:n])
    solved = solved_ref[...]
    small_ref[0:n] = exact_dot(solved, solved, NT)
    for k in range(parts_ref.shape[0]):
        col_sum = jnp.sum(parts_ref[k] * solved, axis=1, keepdims=True)
        small_ref[n + k : n + k + 1] = jnp.transpose(jnp.broadcast_to(col_sum, (n, n)))[0:1]


def time_inverse_kernel(small_ref, pgram_ref, pscale_ref, gram_ref, scale_ref, inverse_ref, *, count):
    n = pgram_ref.shape[0]
    raw = small_ref[0:n]
    row, col = unit_scales(raw, count)
    gram = col * raw * row
    gram_ref[...] = gram
    scale_ref[...] = jnp.concatenate([row * pscale_ref[...], row], axis=0)
    inverse_ref[...] = spd_inverse(with_ridge(pgram_ref[...] * gram))


def shape(*dims):
    return jax.ShapeDtypeStruct(dims, F32)


def call(kernel, outs, *args, flops=10**6, spaces=None, limit=8, scratch=()):
    spaces = spaces or [pltpu.VMEM] * len(args)
    return pl.pallas_call(
        kernel,
        out_shape=outs,
        in_specs=[pl.BlockSpec(memory_space=space) for space in spaces],
        out_specs=[pl.BlockSpec(memory_space=pltpu.VMEM)] * len(outs),
        scratch_shapes=scratch,
        cost_estimate=pl.CostEstimate(flops=flops, bytes_accessed=10**6, transcendentals=0),
        compiler_params=pltpu.CompilerParams(vmem_limit_bytes=limit << 20),
    )(*args)


def swap(x, axis, mask):
    n = lax.axis_size(axis)
    return lax.ppermute(x, axis, [(i, i ^ mask) for i in range(n)])


def masks_of(n):
    return [1 << i for i in range(n.bit_length() - 1)]


def per_device(tensor, level_init, time_init):
    steps, points, levels = tensor.shape
    rank = level_init.shape[0]
    npts, nvar = lax.axis_size("pts"), lax.axis_size("var")
    points_all, levels_all = points * npts, levels * nvar
    pts_masks, var_masks = masks_of(npts), masks_of(nvar)
    half = levels // 2
    flops = 2 * steps * points * levels * rank
    V, S = pltpu.VMEM, pltpu.SMEM
    dma_sems = pltpu.SemaphoreType.DMA((steps,))
    square = shape(rank, rank)
    tensor_hbm = pltpu.with_memory_space_constraint(tensor, pltpu.HBM)
    side = (lax.axis_index("pts") & 1).astype(jnp.int32)[None]

    def sum_over(x, axis, masks):
        for mask in masks:
            x = x + swap(x, axis, mask)
        return x

    (gram,) = call(gram_kernel, [square], level_init)
    gram = sum_over(gram, "var", var_masks)
    (first,) = call(
        first_pass_kernel, [shape(steps, rank, points)], level_init, tensor_hbm,
        flops=flops, limit=24, spaces=[V, pltpu.HBM],
        scratch=[V(tensor.shape, tensor.dtype), dma_sems],
    )
    time = time_init
    mine, tgram, system = call(first_combine_kernel, [shape(rank, points), square, square], gram, time, time.T, first)
    for sweep in range(SWEEPS):
        mine = sum_over(mine, "var", var_masks[:-1])
        other = swap(mine, "var", var_masks[-1])
        inverse, held = call(
            inverse_kernel, [square, V(tensor.shape, tensor.dtype)], system, tensor_hbm,
            flops=flops, limit=24, spaces=[V, pltpu.HBM], scratch=[dma_sems],
        )
        held = pltpu.with_memory_space_constraint(held, V)
        point_solved, parts, keep, send = call(
            level_pass_kernel,
            [shape(rank, points), shape(steps, rank, levels)] + [shape(rank + 8, half)] * 2,
            side, inverse, mine, other, time.T, held,
            flops=flops, limit=24, spaces=[S] + [V] * 5,
            scratch=[V((2, rank, half), F32)],
        )
        keep = keep + swap(send, "pts", pts_masks[0])
        keep = sum_over(keep, "pts", pts_masks[1:])
        other = swap(keep, "pts", pts_masks[0])
        weights, pgram, pscale = call(
            functools.partial(level_weights_kernel, count=points_all),
            [square, square, shape(1, rank)], keep, tgram,
            flops=10**7,
        )
        level_solved, small = call(
            level_solve_kernel, [shape(rank, levels), shape(rank + steps, rank)],
            side, weights, keep, other, parts,
            spaces=[S] + [V] * 4,
        )
        small = sum_over(small, "var", var_masks)
        products = small[rank:]
        gram, scale, inverse = call(
            functools.partial(time_inverse_kernel, count=levels_all),
            [square, shape(2, rank), square], small, pgram, pscale,
            flops=10**7,
        )
        for i, mask in enumerate(pts_masks):
            products2 = swap(products, "pts", mask)
            if i + 1 < len(pts_masks):
                products = products + products2
        if sweep + 1 < SWEEPS:
            pieces, first = [], 0
            for count in PIECES:
                pieces += call(
                    functools.partial(point_pass_kernel, first=first), [shape(count, rank, points)],
                    level_solved, held,
                    flops=flops * count // steps, limit=24,
                )
                first += count
            mine, tgram, system, time = call(
                combine_kernel, [shape(rank, points), square, square, shape(steps, rank)],
                gram, scale, inverse, products, products2, *pieces,
            )
    (time_out,) = call(
        functools.partial(last_time_kernel, factor=math.sqrt(points_all * levels_all)), [shape(steps, rank)],
        scale, inverse, products, products2,
    )
    return (point_solved * pscale[0][:, None], level_solved * scale[1][:, None], time_out)


def solution(mesh):
    placed = (P(None, "pts", "var"), P(None, "var"), P())
    return jax.shard_map(
        per_device,
        mesh=mesh,
        in_specs=placed,
        out_specs=(P(None, "pts"), P(None, "var"), P()),
        check_vma=False,
    )
```
